32 devices in a mesh: band: 4 (over y, core), col: 8 (over z, x).
Axes of the slice: x: 2, y: 2, z: 4, core: 2. Of those that a mesh axis runs over, the one named last changes fastest.
Arguments:
- source: bfloat16 [6, 524288], P(None, ('band', 'col')), may hold values from -6 to 6
- weights: bfloat16 [8192, 128, 128], P(('band', 'col')), may hold values from -0.5 to 0.5
- source_block: int32 [8192], P(('band', 'col')), may hold values from 0 to 127
- owner_device: int32 [8192, 1], P(('band', 'col')), may hold values from 0 to 31, as said below
- target_tile: int32 [8192], P(('band', 'col')), may hold values from 0 to 112, as said below
- cutoff: int32 [64], P(('band', 'col')), may hold values from 1 to 511
Outputs:
- remapped: float32 [6, 64, 7200], P(None, 'band', 'col')
- filtered: float32 [6, 64, 7200], P(None, 'band', 'col')
The draws below stay inside these ranges and needn't reach their ends.
Inputs may be any that keep to these rules, and one draw needn't show every extreme that they name: `owner_device`: owners are numbered band index times 8 plus col index. A device's blocks go only to owners in its own band or in the bands next to it. Among the 256 blocks of one device at most 24 share an owner; in every device exactly 24 do for some owner of its own band, and exactly 24 for some owner of each band next to its own; every device sends at least 15 blocks to each owner of its own band. `target_tile`: every tile of every owner receives at least one block.
All inputs are finite; a program needn't handle non-finite values.
Results may differ from the reference program's by a relative error of at most 0.0003.
Values sent between devices are 32-bit elements; how exact they have to be, the bound alone decides.
A program may use at most 64 MiB of HBM per device.

```python
import jax
import jax.numpy as jnp
from jax import lax

NLON = 7200
BLK = 128
LEV = 6
KW = 512
NB = 256
SB = 128
LATB = 16
NLAT = 64
LON_DEV = 900
TILES_DEV = 113
REG = 15
CAP = 24
NBLOCKS = 8192
NSRC = 524288
N_BAND = 4
N_COL = 8
DEVICES = 32


def remap_layout(key):
    slot_total = 3 * N_COL * CAP
    slots = jnp.arange(slot_total, dtype=jnp.int32)
    offset = slots // (N_COL * CAP)
    owner_col = slots // CAP % N_COL
    within = slots % CAP
    shifts = jax.random.randint(jax.random.fold_in(key, 11), (DEVICES,), 0, TILES_DEV).astype(jnp.int32)

    def one_device(device):
        device_key = jax.random.fold_in(jax.random.fold_in(key, 17), device)
        band = device // N_COL
        column = device % N_COL
        owner_band = band + offset - 1
        valid = (owner_band >= 0) & (owner_band < N_BAND)
        regular = (offset == 1) & (within < REG)
        candidate = valid & ((offset != 1) | (within >= REG))
        forced_cols = jax.random.randint(jax.random.fold_in(device_key, 1), (3,), 0, N_COL).astype(jnp.int32)
        forced = candidate & (owner_col == forced_cols[offset])
        ranking = jax.random.permutation(jax.random.fold_in(device_key, 2), slot_total).astype(jnp.int32)
        score = jnp.where(regular, 0, jnp.where(forced, 1, jnp.where(candidate, 2 + ranking, 4 * slot_total + 4)))
        chosen = jnp.argsort(score, stable=True)[:NB].astype(jnp.int32)
        mixing = jax.random.permutation(jax.random.fold_in(device_key, 3), NB).astype(jnp.int32)
        chosen = chosen[mixing]
        owners = (owner_band[chosen] * N_COL + owner_col[chosen]).astype(jnp.int32)
        random_tile = jax.random.randint(jax.random.fold_in(device_key, 4), (NB,), 0, TILES_DEV).astype(jnp.int32)
        regular_tile = (column * REG + within[chosen] + shifts[owners]) % TILES_DEV
        tiles = jnp.where(regular[chosen], regular_tile, random_tile).astype(jnp.int32)
        return (owners, tiles)
    owners, tiles = jax.vmap(one_device)(jnp.arange(DEVICES, dtype=jnp.int32))
    return (owners.reshape(NBLOCKS, 1).astype(jnp.int32), tiles.reshape(NBLOCKS).astype(jnp.int32))


def draw_owner_device(key, part):
    return remap_layout(jax.random.fold_in(key, 5))[0]


def draw_target_tile(key, part):
    return remap_layout(jax.random.fold_in(key, 5))[1]


def place_ends(array, key, low, high):
    place = [jax.random.randint(jax.random.fold_in(key, axis), (), 0, length) for axis, length in enumerate(array.shape)]
    longest = array.shape.index(max(array.shape))
    beside = place[:longest] + [(place[longest] + 1) % array.shape[longest]] + place[longest + 1:]
    return array.at[tuple(place)].set(low).at[tuple(beside)].set(high)


def levels(rng, dims, pieces, low, largest):
    factor_of, own = 1.0, jax.random.fold_in(rng, 6)
    for position, parts in pieces:
        draws = jnp.exp(jax.random.uniform(jax.random.fold_in(own, position), (parts,), jnp.float32, low / len(pieces), largest / len(pieces)))
        factor_of = factor_of * jnp.repeat(draws, dims[position] // parts).reshape([-1 if axis == position else 1 for axis in range(len(dims))])
    return factor_of


def centred(own_key, dims, width, most, split=(), kind=jnp.bfloat16):
    gain = levels(own_key, dims, split, -0.22, 0.18) if split else 1.0
    result = jax.random.normal(own_key, dims, jnp.float32) * width * gain
    return jnp.minimum(jnp.maximum(result, -most), most).astype(kind)


def setup_inputs(seed: int = 0) -> dict:
    splits = jax.random.split(jax.random.key(seed), 7)
    source = centred(splits[0], (LEV, NSRC), 1.0, 6.0, ((1, 32),))
    weights = centred(splits[1], (NBLOCKS, BLK, BLK), BLK ** -0.5, 0.5, ((0, 32),))
    source_block = place_ends(jax.random.randint(splits[2], (NBLOCKS,), 0, SB), jax.random.fold_in(splits[2], 1), 0, SB - 1).astype(jnp.int32)
    owner_device = draw_owner_device(jax.random.fold_in(splits[6], 71), 0)
    target_tile = draw_target_tile(jax.random.fold_in(splits[6], 71), 0)
    cutoff = place_ends(jax.random.randint(splits[5], (NLAT,), 1, KW), jax.random.fold_in(splits[5], 1), 1, KW - 1).astype(jnp.int32)
    return {"source": source, "weights": weights, "source_block": source_block, "owner_device": owner_device, "target_tile": target_tile, "cutoff": cutoff}


TWO_PI = 6.283185307179586


def zonal_table(start_index, length, period, wave_count):
    positions = start_index + lax.broadcasted_iota(jnp.int32, (length, wave_count), 0)
    wave_index = lax.broadcasted_iota(jnp.int32, (length, wave_count), 1)
    phases = (positions * wave_index) % period
    angles = phases.astype(jnp.float32) * (TWO_PI / period)
    return jnp.concatenate([jnp.cos(angles), jnp.sin(angles)], axis=1)


def spectral_weights(cutoffs, wave_count, period):
    wave_index = lax.broadcasted_iota(jnp.int32, (cutoffs.shape[0], wave_count), 1)
    scaled = jnp.where(wave_index == 0, 1.0, 2.0) / period
    retained = jnp.where(wave_index <= cutoffs[:, None], scaled, 0.0).astype(jnp.float32)
    return jnp.concatenate([retained, retained], axis=1)


def reference(source, weights, source_block, owner_device, target_tile, cutoff):
    device_total = N_BAND * N_COL
    blocks_all = source.reshape(LEV, device_total * SB, BLK)
    owners_all = owner_device[:, 0]

    def add_device(totals, device_index):
        first_block = device_index * NB
        block_weights = lax.dynamic_slice_in_dim(weights, first_block, NB, 0)
        chosen = lax.dynamic_slice_in_dim(source_block, first_block, NB, 0)
        owners = lax.dynamic_slice_in_dim(owners_all, first_block, NB, 0)
        tiles_hit = lax.dynamic_slice_in_dim(target_tile, first_block, NB, 0)
        picked = jnp.take(blocks_all, (device_index * SB + chosen).astype(jnp.int32), axis=1)
        partial_value = jnp.einsum("lnb,nbt->nlt", picked.astype(jnp.float32), block_weights.astype(jnp.float32))
        totals = totals.at[(owners * TILES_DEV + tiles_hit).astype(jnp.int32)].add(partial_value)
        return totals, None

    totals, unused = lax.scan(add_device, jnp.zeros((device_total * TILES_DEV, LEV, BLK), jnp.float32), jnp.arange(device_total, dtype=jnp.int32))
    cell_count = LATB * LON_DEV
    tiles = totals.reshape(N_BAND, N_COL, TILES_DEV, LEV, BLK)
    tiles = jnp.transpose(tiles, (3, 0, 1, 2, 4)).reshape(LEV, N_BAND, N_COL, TILES_DEV * BLK)[:, :, :, :cell_count]
    tiles = tiles.reshape(LEV, N_BAND, N_COL, LATB, LON_DEV)
    remapped = jnp.transpose(tiles, (0, 1, 3, 2, 4)).reshape(LEV, NLAT, NLON)
    wave_table = zonal_table(0, NLON, NLON, KW)
    spectrum = jnp.dot(remapped.reshape(LEV * NLAT, NLON), wave_table, precision=lax.Precision.HIGHEST, preferred_element_type=jnp.float32)
    spectrum = spectrum.reshape(LEV, NLAT, 2 * KW) * spectral_weights(cutoff, KW, NLON)[None]
    filtered = jnp.dot(spectrum.reshape(LEV * NLAT, 2 * KW), wave_table.T, precision=lax.Precision.HIGHEST, preferred_element_type=jnp.float32)
    return remapped, filtered.reshape(LEV, NLAT, NLON)
```

```python
import functools

import jax
import jax.numpy as jnp
from jax import lax
from jax.experimental import pallas as pl
from jax.experimental.pallas import tpu as pltpu
from jax.sharding import PartitionSpec as P

NLON = 7200
KW = 512
LANES = 128
STEP = 16
TWO_PI = 6.283185307179586
MESH = pl.DeviceIdType.MESH
F32 = jnp.float32
BF16 = jnp.bfloat16


def round_up(value, multiple):
    return (value + multiple - 1) // multiple * multiple


def split(value):
    high = value.astype(BF16)
    return high, (value - high.astype(F32)).astype(BF16)


def dot(left, right, left_dim=1, right_dim=0):
    return lax.dot_general(
        left, right, (((left_dim,), (right_dim,)), ((), ())), preferred_element_type=F32
    )


def exchange_kernel(
    bands, cols, levels, capacity, wave_count,
    partial, owner_row, owner_column, tile_row, fine, coarse,
    sums, table_high, table_low,
    slab, recv, send_sem, recv_sem,
):
    band, col = lax.axis_index("band"), lax.axis_index("col")
    blocks = partial.shape[0]
    rows = levels * capacity
    owners = owner_row[...]
    sublane = lax.broadcasted_iota(jnp.int32, (blocks, blocks), 0)
    lane = lax.broadcasted_iota(jnp.int32, (blocks, blocks), 1)
    earlier = (owner_column[...] == owners) & (sublane < lane)
    rank = jnp.sum(earlier.astype(jnp.int32), axis=0, keepdims=True)
    place = owners - (band - 1) * cols
    slot = place * capacity + rank
    data = jnp.concatenate([partial[:, level, :] for level in range(levels)], axis=1)
    stacked = jnp.concatenate(split(data), axis=0)
    slot_lane = lax.broadcasted_iota(jnp.int32, (LANES, blocks), 0)
    tile_at = jnp.where(slot_lane == rank, tile_row[...], 0).astype(F32).astype(BF16)

    def valid(offset):
        target = band + (offset - 1)
        return (target >= 0) & (target < bands)

    def send(offset):
        group = cols * capacity
        ids = lax.broadcasted_iota(jnp.int32, (group, blocks), 0) + offset * group
        placing = (ids == slot).astype(F32).astype(BF16)
        placed = dot(jnp.concatenate([placing, placing], axis=1), stacked)
        place_ids = lax.broadcasted_iota(jnp.int32, (cols, blocks), 0) + offset * cols
        chosen = (place_ids == place).astype(F32).astype(BF16)
        tags = dot(chosen, tile_at, 1, 1)
        here = pl.ds(offset * cols, cols)
        for level in range(levels):
            piece = placed[:, level * LANES : (level + 1) * LANES]
            slab[here, level * capacity : (level + 1) * capacity, :] = piece.reshape(
                cols, capacity, LANES
            )
        slab[here, rows : rows + 8, :] = jnp.broadcast_to(tags[:, None, :], (cols, 8, LANES))

        def one(step, carry):
            to = lax.rem(col + cols // 2 + step, cols)

            def start_remote():
                pltpu.make_async_remote_copy(
                    src_ref=slab.at[offset * cols + to],
                    dst_ref=recv.at[(2 - offset) * cols + col],
                    send_sem=send_sem.at[offset],
                    recv_sem=recv_sem.at[2 - offset],
                    device_id=(band + (offset - 1), to),
                    device_id_type=MESH,
                ).start()

            if offset == 1:
                pl.when(to != col)(start_remote)
            else:
                start_remote()
            return carry

        lax.fori_loop(0, cols, one, 0)
        if offset == 1:
            pltpu.make_async_copy(
                slab.at[cols + col], recv.at[cols + col], recv_sem.at[1]
            ).start()

    for offset in (0, 2, 1):
        pl.when(valid(offset))(functools.partial(send, offset))

    def table_step(step, carry):
        pair = coarse[step]
        cos_base, sin_base = pair[0:1], pair[1:2]
        cos_fine, sin_fine = fine[0], fine[1]
        at = pl.ds(pl.multiple_of(step * STEP, STEP), STEP)
        for start, value in (
            (0, cos_base * cos_fine - sin_base * sin_fine),
            (wave_count, sin_base * cos_fine + cos_base * sin_fine),
        ):
            high, low = split(value)
            table_high[at, start : start + wave_count] = high
            table_low[at, start : start + wave_count] = low
        return carry

    lax.fori_loop(0, coarse.shape[0], table_step, 0)

    tiles = sums.shape[1]
    sums[...] = jnp.zeros_like(sums)

    def receive(offset):
        here = pl.ds(offset * cols, cols)
        pltpu.make_async_copy(slab.at[here], recv.at[here], recv_sem.at[offset]).wait()
        tags = jnp.transpose(recv[here, rows, :])
        wide = lax.broadcasted_iota(jnp.int32, (capacity, tiles), 1).astype(F32)
        chooser = jnp.concatenate(
            [
                (tags[:capacity, source : source + 1] == wide).astype(F32)
                for source in range(cols)
            ],
            axis=0,
        )
        chooser = jnp.transpose(chooser).astype(BF16)
        arrived = jnp.concatenate(
            [
                recv[here, level * capacity : (level + 1) * capacity, :].reshape(
                    cols * capacity, LANES
                )
                for level in range(levels)
            ],
            axis=1,
        )
        high, low = split(arrived)
        total = dot(chooser, high) + dot(chooser, low)
        for level in range(levels):
            sums[level] += total[:, level * LANES : (level + 1) * LANES]

    for offset in (1, 0, 2):
        pl.when(valid(offset))(functools.partial(receive, offset))

    def drain(offset):
        first = offset * cols
        count = cols - 1 if offset == 1 else cols
        here = pl.ds(first, count)
        pltpu.make_async_copy(slab.at[here], recv.at[here], send_sem.at[offset]).wait()

    for offset in range(3):
        pl.when(valid(offset))(functools.partial(drain, offset))


def exchange(mesh, capacity, tiles, long_pad, partial, owner, tile, fine, coarse):
    bands, cols = mesh.shape["band"], mesh.shape["col"]
    blocks, levels, width = partial.shape
    wave_count = fine.shape[-1]
    slab_rows = levels * capacity + 8
    vmem = pl.BlockSpec(memory_space=pltpu.VMEM)
    return pl.pallas_call(
        functools.partial(exchange_kernel, bands, cols, levels, capacity, wave_count),
        out_shape=(
            jax.ShapeDtypeStruct((levels, tiles, width), F32),
            jax.ShapeDtypeStruct((long_pad, 2 * wave_count), BF16),
            jax.ShapeDtypeStruct((long_pad, 2 * wave_count), BF16),
        ),
        in_specs=[vmem] * 6,
        out_specs=(vmem,) * 3,
        scratch_shapes=[
            pltpu.VMEM((3 * cols, slab_rows, width), F32),
            pltpu.VMEM((3 * cols, slab_rows, width), F32),
            pltpu.SemaphoreType.DMA((3,)),
            pltpu.SemaphoreType.DMA((3,)),
        ],
        compiler_params=pltpu.CompilerParams(has_side_effects=True, vmem_limit_bytes=48 << 20),
    )(partial, owner.reshape(1, blocks), owner, tile.reshape(1, blocks), fine, coarse)


def filter_kernel(
    cols, group, lat_here, period, wave_count,
    cutoff, field, table_high, table_low,
    out,
    spectra, arrived, scaled, gathered, send_sem, recv_sem, send_sem2, recv_sem2,
):
    band, col = lax.axis_index("band"), lax.axis_index("col")
    rows = cols * group
    width_tiles = spectra.shape[1]
    high, low = split(field[...])
    both = dot(jnp.concatenate([high, low], axis=0), table_high[...])
    spectrum = both[:rows] + both[rows:] + dot(high, table_low[...])
    for tile in range(width_tiles):
        spectra[:, tile, :] = spectrum[:, tile * LANES : (tile + 1) * LANES]

    def mine(ref, index):
        return ref.at[pl.ds(index * group, group)]

    def scatter(step, carry):
        to = lax.rem(col + cols // 2 + step, cols)

        def start_remote():
            pltpu.make_async_remote_copy(
                src_ref=mine(spectra, to),
                dst_ref=mine(arrived, col),
                send_sem=send_sem,
                recv_sem=recv_sem,
                device_id=(band, to),
                device_id_type=MESH,
            ).start()

        pl.when(to != col)(start_remote)
        return carry

    lax.fori_loop(0, cols, scatter, 0)
    pltpu.make_async_copy(mine(spectra, col), mine(arrived, col), recv_sem).start()
    j = (
        lax.broadcasted_iota(jnp.int32, (width_tiles, LANES), 0) * LANES
        + lax.broadcasted_iota(jnp.int32, (width_tiles, LANES), 1)
    )
    wave = jnp.where(j >= wave_count, j - wave_count, j)
    weight = jnp.where(wave == 0, 1.0, 2.0) / period
    gains = [jnp.where(wave <= cutoff[lat], weight, 0.0).astype(F32) for lat in range(lat_here)]
    pltpu.make_async_copy(spectra, arrived, recv_sem).wait()
    for row in range(group):
        total = arrived[row]
        for source in range(1, cols):
            total += arrived[source * group + row]
        scaled[row] = total * gains[row % lat_here]

    def spread(step, carry):
        to = lax.rem(col + cols // 2 + step, cols)

        def start_remote():
            pltpu.make_async_remote_copy(
                src_ref=scaled,
                dst_ref=mine(gathered, col),
                send_sem=send_sem2,
                recv_sem=recv_sem2,
                device_id=(band, to),
                device_id_type=MESH,
            ).start()

        pl.when(to != col)(start_remote)
        return carry

    lax.fori_loop(0, cols, spread, 0)
    pltpu.make_async_copy(scaled, mine(gathered, col), recv_sem2).start()
    pltpu.make_async_copy(spectra, gathered, recv_sem2).wait()
    spectrum = jnp.concatenate([gathered[:, tile, :] for tile in range(width_tiles)], axis=1)
    high, low = split(spectrum)
    both = dot(jnp.concatenate([high, low], axis=0), table_high[...], 1, 1)
    out[...] = both[:rows] + both[rows:] + dot(high, table_low[...], 1, 1)
    others = pl.ds(0, (cols - 1) * group)
    pltpu.make_async_copy(spectra.at[others], arrived.at[others], send_sem).wait()
    pltpu.make_async_copy(spectra.at[others], arrived.at[others], send_sem2).wait()


def zonal_filter(mesh, group, cutoff, field, table_high, table_low):
    cols = mesh.shape["col"]
    rows, long_pad = field.shape
    waves = table_high.shape[1]
    shape = (rows, waves // LANES, LANES)
    vmem = pl.BlockSpec(memory_space=pltpu.VMEM)
    return pl.pallas_call(
        functools.partial(filter_kernel, cols, group, cutoff.shape[0], NLON, waves // 2),
        out_shape=jax.ShapeDtypeStruct((rows, long_pad), F32),
        in_specs=[pl.BlockSpec(memory_space=pltpu.SMEM)] + [vmem] * 3,
        out_specs=vmem,
        scratch_shapes=[
            pltpu.VMEM(shape, F32),
            pltpu.VMEM(shape, F32),
            pltpu.VMEM((group,) + shape[1:], F32),
            pltpu.VMEM(shape, F32),
            pltpu.SemaphoreType.DMA,
            pltpu.SemaphoreType.DMA,
            pltpu.SemaphoreType.DMA,
            pltpu.SemaphoreType.DMA,
        ],
        compiler_params=pltpu.CompilerParams(has_side_effects=True, vmem_limit_bytes=48 << 20),
    )(cutoff, field, table_high, table_low)


def cos_sin(positions):
    wave_index = lax.broadcasted_iota(jnp.int32, (positions.shape[0], KW), 1)
    phases = positions[:, None] * wave_index % NLON
    angles = phases.astype(F32) * (TWO_PI / NLON)
    return jnp.cos(angles), jnp.sin(angles)


def local(mesh, source, weights, source_block, owner_device, target_tile, cutoff):
    cols = mesh.shape["col"]
    levels = source.shape[0]
    block_count, block_width = weights.shape[:2]
    lat_here = cutoff.shape[0]
    lat_band = lat_here * cols
    longitudes = NLON // cols
    cell_count = lat_band * longitudes
    tile_count = (cell_count + block_width - 1) // block_width
    regular = (tile_count + cols - 1) // cols
    capacity = regular + max(1, (block_count - cols * regular + 2 * cols - 1) // (2 * cols))
    capacity = round_up(capacity, 8)
    tiles = round_up(tile_count, LANES)
    long_pad = round_up(longitudes, LANES)
    fine = jnp.stack(cos_sin(jnp.arange(STEP, dtype=jnp.int32)))
    starts = lax.axis_index("col") * longitudes + STEP * jnp.arange(long_pad // STEP, dtype=jnp.int32)
    coarse = jnp.stack(cos_sin(starts), axis=1)

    blocks_here = source.reshape(levels, -1, block_width)
    picked = jnp.take(blocks_here, source_block, axis=1)
    partial = jnp.einsum("lnb,nbt->nlt", picked, weights, preferred_element_type=F32)
    sums, table_high, table_low = exchange(
        mesh, capacity, tiles, long_pad, partial, owner_device, target_tile, fine, coarse
    )
    remapped = sums.reshape(levels, -1)[:, :cell_count].reshape(levels, lat_band, longitudes)
    group = levels * lat_here
    field = remapped.reshape(levels, cols, lat_here, longitudes).transpose(1, 0, 2, 3)
    field = field.reshape(cols * group, longitudes)
    field = jnp.pad(field, ((0, 0), (0, long_pad - longitudes)))
    filtered = zonal_filter(mesh, group, cutoff, field, table_high, table_low)
    filtered = filtered[:, :longitudes].reshape(cols, levels, lat_here, longitudes)
    filtered = filtered.transpose(1, 0, 2, 3).reshape(levels, lat_band, longitudes)
    return remapped, filtered


def solution(mesh):
    in_specs = (
        P(None, ("band", "col")),
        P(("band", "col"), None, None),
        P(("band", "col")),
        P(("band", "col"), None),
        P(("band", "col")),
        P(("band", "col")),
    )
    out_specs = (P(None, "band", "col"), P(None, "band", "col"))
    return jax.shard_map(
        functools.partial(local, mesh),
        mesh=mesh,
        in_specs=in_specs,
        out_specs=out_specs,
        check_vma=False,
    )
```

```python
import functools

import jax
import jax.numpy as jnp
import numpy as np
from jax import lax
from jax.experimental import pallas as pl
from jax.experimental.pallas import tpu as pltpu
from jax.sharding import PartitionSpec as P

NLON = 7200
KW = 512
LANES = 128
STEP = 16
MESH = pl.DeviceIdType.MESH
F32 = jnp.float32
BF16 = jnp.bfloat16


def round_up(value, multiple):
    return (value + multiple - 1) // multiple * multiple


def split(value):
    high = value.astype(BF16)
    return high, (value - high.astype(F32)).astype(BF16)


def dot(left, right, left_dim=1, right_dim=0):
    return lax.dot_general(
        left, right, (((left_dim,), (right_dim,)), ((), ())), preferred_element_type=F32
    )


def remap_kernel(
    bands, cols, levels, capacity, wave_count, period, longitudes,
    cutoff, partial, owner_row, owner_column, tile_row, fine, coarse, start,
    remapped, filtered,
    sums, table_high, table_low, rotated, field, slab, recv,
    spectra, arrived, scaled, gathered,
    send_sem, recv_sem, scatter_send, scatter_recv, spread_send, spread_recv,
):
    band, col = lax.axis_index("band"), lax.axis_index("col")
    blocks = partial.shape[0]
    rows = levels * capacity
    owners = owner_row[...]
    sublane = lax.broadcasted_iota(jnp.int32, (blocks, blocks), 0)
    lane = lax.broadcasted_iota(jnp.int32, (blocks, blocks), 1)
    earlier = (owner_column[...] == owners) & (sublane < lane)
    rank = jnp.sum(earlier.astype(jnp.int32), axis=0, keepdims=True)
    place = owners - (band - 1) * cols
    slot = place * capacity + rank
    data = jnp.concatenate([partial[:, level, :] for level in range(levels)], axis=1)
    stacked = jnp.concatenate(split(data), axis=0)
    slot_lane = lax.broadcasted_iota(jnp.int32, (LANES, blocks), 0)
    tile_at = jnp.where(slot_lane == rank, tile_row[...], 0).astype(F32).astype(BF16)

    def valid(offset):
        target = band + (offset - 1)
        return (target >= 0) & (target < bands)

    def to_others(start_copy):
        def one(step, carry):
            to = lax.rem(col + cols // 2 + step, cols)
            pl.when(to != col)(functools.partial(start_copy, to))
            return carry

        lax.fori_loop(0, cols, one, 0)

    def send(offset):
        group = cols * capacity
        ids = lax.broadcasted_iota(jnp.int32, (group, blocks), 0) + offset * group
        placing = (ids == slot).astype(F32).astype(BF16)
        placed = dot(jnp.concatenate([placing, placing], axis=1), stacked)
        place_ids = lax.broadcasted_iota(jnp.int32, (cols, blocks), 0) + offset * cols
        chosen = (place_ids == place).astype(F32).astype(BF16)
        tags = dot(chosen, tile_at, 1, 1)
        here = pl.ds(offset * cols, cols)
        for level in range(levels):
            piece = placed[:, level * LANES : (level + 1) * LANES]
            slab[here, level * capacity : (level + 1) * capacity, :] = piece.reshape(
                cols, capacity, LANES
            )
        slab[here, rows : rows + 8, :] = jnp.broadcast_to(tags[:, None, :], (cols, 8, LANES))

        def start_remote(to):
            pltpu.make_async_remote_copy(
                src_ref=slab.at[offset * cols + to],
                dst_ref=recv.at[(2 - offset) * cols + col],
                send_sem=send_sem.at[offset],
                recv_sem=recv_sem.at[2 - offset],
                device_id=(band + (offset - 1), to),
                device_id_type=MESH,
            ).start()

        to_others(start_remote)
        if offset == 1:
            pltpu.make_async_copy(
                slab.at[cols + col], recv.at[cols + col], recv_sem.at[1]
            ).start()
        else:
            start_remote(col)

    for offset in (0, 2, 1):
        pl.when(valid(offset))(functools.partial(send, offset))

    begin = start[col]
    cos_start, sin_start = begin[0:1], begin[1:2]
    rotated[0] = fine[0] * cos_start - fine[1] * sin_start
    rotated[1] = fine[1] * cos_start + fine[0] * sin_start

    def table_step(step, carry):
        pair = coarse[step]
        cos_base, sin_base = pair[0:1], pair[1:2]
        cos_fine, sin_fine = rotated[0], rotated[1]
        at = pl.ds(pl.multiple_of(step * STEP, STEP), STEP)
        for first, value in (
            (0, cos_base * cos_fine - sin_base * sin_fine),
            (wave_count, sin_base * cos_fine + cos_base * sin_fine),
        ):
            high, low = split(value)
            table_high[at, first : first + wave_count] = high
            table_low[at, first : first + wave_count] = low
        return carry

    lax.fori_loop(0, coarse.shape[0], table_step, 0)

    tiles = sums.shape[1]
    sums[...] = jnp.zeros_like(sums)

    def receive(offset):
        here = pl.ds(offset * cols, cols)
        pltpu.make_async_copy(slab.at[here], recv.at[here], recv_sem.at[offset]).wait()
        tags = jnp.transpose(recv[here, rows, :])
        wide = lax.broadcasted_iota(jnp.int32, (capacity, tiles), 1).astype(F32)
        chooser = jnp.concatenate(
            [
                (tags[:capacity, source : source + 1] == wide).astype(F32)
                for source in range(cols)
            ],
            axis=0,
        )
        chooser = jnp.transpose(chooser).astype(BF16)
        incoming = jnp.concatenate(
            [
                recv[here, level * capacity : (level + 1) * capacity, :].reshape(
                    cols * capacity, LANES
                )
                for level in range(levels)
            ],
            axis=1,
        )
        high, low = split(incoming)
        total = dot(chooser, high) + dot(chooser, low)
        for level in range(levels):
            sums[level] += total[:, level * LANES : (level + 1) * LANES]

    for offset in (0, 2, 1):
        pl.when(valid(offset))(functools.partial(receive, offset))

    long_tiles, field_rows = field.shape[:2]
    lat_band = field_rows // levels
    shape3 = (levels, long_tiles, LANES)
    lane3 = lax.broadcasted_iota(jnp.int32, shape3, 2)
    inside = lax.broadcasted_iota(jnp.int32, shape3, 1) * LANES + lane3 < longitudes
    for lat in range(lat_band):
        first, shift = divmod(lat * longitudes, LANES)
        value = sums[:, first : first + long_tiles, :]
        if shift:
            after = sums[:, first + 1 : first + 1 + long_tiles, :]
            value = jnp.where(
                lane3 < LANES - shift,
                pltpu.roll(value, LANES - shift, 2),
                pltpu.roll(after, LANES - shift, 2),
            )
        value = jnp.where(inside, value, 0.0)
        for level in range(levels):
            field[:, level * lat_band + lat, :] = value[level]

    rows_wide = jnp.concatenate([field[tile] for tile in range(long_tiles)], axis=1)
    high, low = split(rows_wide)
    both = dot(jnp.concatenate([high, low], axis=0), table_high[...])
    spectrum = both[:field_rows] + both[field_rows:] + dot(high, table_low[...])
    wave_tiles = spectra.shape[2]
    lat_here = lat_band // cols
    for tile in range(wave_tiles):
        spectra[:, :, tile, :] = spectrum[:, tile * LANES : (tile + 1) * LANES].reshape(
            levels, lat_band, LANES
        )

    def lats(ref, index):
        return ref.at[:, pl.ds(index * lat_here, lat_here)]

    def scatter(to):
        pltpu.make_async_remote_copy(
            src_ref=lats(spectra, to),
            dst_ref=arrived.at[col],
            send_sem=scatter_send,
            recv_sem=scatter_recv,
            device_id=(band, to),
            device_id_type=MESH,
        ).start()

    to_others(scatter)
    pltpu.make_async_copy(lats(spectra, col), arrived.at[col], scatter_recv).start()
    remapped[...] = rows_wide[:, :longitudes].reshape(levels, lat_band, longitudes)
    j = (
        lax.broadcasted_iota(jnp.int32, (wave_tiles, LANES), 0) * LANES
        + lax.broadcasted_iota(jnp.int32, (wave_tiles, LANES), 1)
    )
    wave = jnp.where(j >= wave_count, j - wave_count, j)
    weight = jnp.where(wave == 0, 1.0, 2.0) / period
    gains = [jnp.where(wave <= cutoff[lat], weight, 0.0).astype(F32) for lat in range(lat_here)]
    pltpu.make_async_copy(arrived, arrived, scatter_recv).wait()
    for level in range(levels):
        for lat in range(lat_here):
            total = arrived[0, level, lat]
            for source in range(1, cols):
                total += arrived[source, level, lat]
            scaled[level, lat] = total * gains[lat]

    def spread(to):
        pltpu.make_async_remote_copy(
            src_ref=scaled,
            dst_ref=lats(gathered, col),
            send_sem=spread_send,
            recv_sem=spread_recv,
            device_id=(band, to),
            device_id_type=MESH,
        ).start()

    to_others(spread)
    pltpu.make_async_copy(scaled, lats(gathered, col), spread_recv).start()

    def drain(offset):
        count = cols - 1 if offset == 1 else cols
        here = pl.ds(offset * cols, count)
        pltpu.make_async_copy(slab.at[here], recv.at[here], send_sem.at[offset]).wait()

    for offset in range(3):
        pl.when(valid(offset))(functools.partial(drain, offset))
    others = arrived.at[pl.ds(0, cols - 1)]
    pltpu.make_async_copy(others, others, scatter_send).wait()

    pltpu.make_async_copy(spectra, gathered, spread_recv).wait()
    spectrum = jnp.concatenate(
        [gathered[:, :, tile, :].reshape(field_rows, LANES) for tile in range(wave_tiles)], axis=1
    )
    high, low = split(spectrum)
    both = dot(jnp.concatenate([high, low], axis=0), table_high[...], 1, 1)
    result = both[:field_rows] + both[field_rows:] + dot(high, table_low[...], 1, 1)
    filtered[...] = result[:, :longitudes].reshape(levels, lat_band, longitudes)
    pltpu.make_async_copy(others, others, spread_send).wait()


def cos_sin(positions):
    phases = positions[:, None] * np.arange(KW)[None, :] % NLON
    angles = phases * (2 * np.pi / NLON)
    return np.cos(angles).astype(np.float32), np.sin(angles).astype(np.float32)


def local(mesh, source, weights, source_block, owner_device, target_tile, cutoff):
    bands, cols = mesh.shape["band"], mesh.shape["col"]
    levels = source.shape[0]
    block_count, block_width = weights.shape[:2]
    lat_here = cutoff.shape[0]
    lat_band = lat_here * cols
    longitudes = NLON // cols
    cell_count = lat_band * longitudes
    tile_count = (cell_count + block_width - 1) // block_width
    regular = (tile_count + cols - 1) // cols
    capacity = regular + max(1, (block_count - cols * regular + 2 * cols - 1) // (2 * cols))
    capacity = round_up(capacity, 8)
    long_pad = round_up(longitudes, LANES)
    long_tiles = long_pad // LANES
    tiles = round_up(tile_count + long_tiles, LANES)
    fine = np.stack(cos_sin(np.arange(STEP)))
    coarse = np.stack(cos_sin(STEP * np.arange(long_pad // STEP)), axis=1)
    start = np.stack(cos_sin(longitudes * np.arange(cols)), axis=1)

    blocks_here = source.reshape(levels, -1, block_width)
    picked = blocks_here.at[:, source_block].get(mode="promise_in_bounds")
    partial = jnp.einsum("lnb,nbt->nlt", picked, weights, preferred_element_type=F32)
    slab_rows = levels * capacity + 8
    wave_tiles = 2 * KW // LANES
    vmem = pl.BlockSpec(memory_space=pltpu.VMEM)
    shape = jax.ShapeDtypeStruct((levels, lat_band, longitudes), F32)
    return pl.pallas_call(
        functools.partial(remap_kernel, bands, cols, levels, capacity, KW, NLON, longitudes),
        out_shape=(shape, shape),
        in_specs=[pl.BlockSpec(memory_space=pltpu.SMEM)] + [vmem] * 7,
        out_specs=(vmem, vmem),
        scratch_shapes=[
            pltpu.VMEM((levels, tiles, LANES), F32),
            pltpu.VMEM((long_pad, 2 * KW), BF16),
            pltpu.VMEM((long_pad, 2 * KW), BF16),
            pltpu.VMEM((2, STEP, KW), F32),
            pltpu.VMEM((long_tiles, levels * lat_band, LANES), F32),
            pltpu.VMEM((3 * cols, slab_rows, LANES), F32),
            pltpu.VMEM((3 * cols, slab_rows, LANES), F32),
            pltpu.VMEM((levels, lat_band, wave_tiles, LANES), F32),
            pltpu.VMEM((cols, levels, lat_here, wave_tiles, LANES), F32),
            pltpu.VMEM((levels, lat_here, wave_tiles, LANES), F32),
            pltpu.VMEM((levels, lat_band, wave_tiles, LANES), F32),
            pltpu.SemaphoreType.DMA((3,)),
            pltpu.SemaphoreType.DMA((3,)),
            pltpu.SemaphoreType.DMA,
            pltpu.SemaphoreType.DMA,
            pltpu.SemaphoreType.DMA,
            pltpu.SemaphoreType.DMA,
        ],
        compiler_params=pltpu.CompilerParams(has_side_effects=True, vmem_limit_bytes=48 << 20),
    )(
        cutoff,
        partial,
        owner_device.reshape(1, block_count),
        owner_device,
        target_tile.reshape(1, block_count),
        fine,
        coarse,
        start,
    )


def solution(mesh):
    in_specs = (
        P(None, ("band", "col")),
        P(("band", "col"), None, None),
        P(("band", "col")),
        P(("band", "col"), None),
        P(("band", "col")),
        P(("band", "col")),
    )
    out_specs = (P(None, "band", "col"), P(None, "band", "col"))
    return jax.shard_map(
        functools.partial(local, mesh),
        mesh=mesh,
        in_specs=in_specs,
        out_specs=out_specs,
        check_vma=False,
    )
```

```python
import functools

import jax
import jax.numpy as jnp
import numpy as np
from jax import lax
from jax.experimental import pallas as pl
from jax.experimental.pallas import tpu as pltpu
from jax.sharding import PartitionSpec as P

NLON = 7200
KW = 512
LANES = 128
STEP = 16
MESH = pl.DeviceIdType.MESH
F32 = jnp.float32
BF16 = jnp.bfloat16


def round_up(value, multiple):
    return (value + multiple - 1) // multiple * multiple


def split(value):
    high = value.astype(BF16)
    return high, (value - high.astype(F32)).astype(BF16)


def dot(left, right, left_dim=1, right_dim=0):
    return lax.dot_general(
        left, right, (((left_dim,), (right_dim,)), ((), ())), preferred_element_type=F32
    )


def remap_kernel(
    bands, cols, levels, capacity, wave_count, period, longitudes, tile_count,
    cutoff, partial, owner_row, tile_row, fine, coarse, start,
    remapped, filtered,
    sums, table_high, table_low, rotated, field, slab, recv, relay, relay_sums, passed,
    spectra, arrived, scaled, gathered,
    send_sem, recv_sem, relay_sem, pass_send, pass_recv,
    scatter_send, scatter_recv, spread_send, spread_recv,
):
    band, col = lax.axis_index("band"), lax.axis_index("col")
    blocks = partial.shape[0]
    rows = levels * capacity
    owners = owner_row[...]
    sublane = lax.broadcasted_iota(jnp.int32, (blocks, blocks), 0)
    lane = lax.broadcasted_iota(jnp.int32, (blocks, blocks), 1)
    owners_wide = jnp.broadcast_to(owners.astype(F32), (8, blocks))
    owner_column = jnp.transpose(owners_wide)[:, 0:1]
    earlier = (owner_column == owners.astype(F32)) & (sublane < lane)
    rank = jnp.sum(earlier.astype(jnp.int32), axis=0, keepdims=True)
    place = owners - (band - 1) * cols
    slot = place * capacity + rank
    data = jnp.concatenate([partial[:, level, :] for level in range(levels)], axis=1)
    stacked = jnp.concatenate(split(data), axis=0)
    slot_lane = lax.broadcasted_iota(jnp.int32, (LANES, blocks), 0)
    tile_at = jnp.where(slot_lane == rank, tile_row[...], 0).astype(F32).astype(BF16)

    def valid(offset):
        target = band + (offset - 1)
        return (target >= 0) & (target < bands)

    def to_others(start_copy):
        def one(step, carry):
            to = lax.rem(col + cols // 2 + step, cols)
            pl.when(to != col)(functools.partial(start_copy, to))
            return carry

        lax.fori_loop(0, cols, one, 0)

    def send(offset):
        group = cols * capacity
        ids = lax.broadcasted_iota(jnp.int32, (group, blocks), 0) + offset * group
        placing = (ids == slot).astype(F32).astype(BF16)
        placed = dot(jnp.concatenate([placing, placing], axis=1), stacked)
        place_ids = lax.broadcasted_iota(jnp.int32, (cols, blocks), 0) + offset * cols
        chosen = (place_ids == place).astype(F32).astype(BF16)
        tags = dot(chosen, tile_at, 1, 1)
        here = pl.ds(offset * cols, cols)
        for level in range(levels):
            piece = placed[:, level * LANES : (level + 1) * LANES]
            slab[here, level * capacity : (level + 1) * capacity, :] = piece.reshape(
                cols, capacity, LANES
            )
        slab[here, rows : rows + 8, :] = jnp.broadcast_to(tags[:, None, :], (cols, 8, LANES))

    half_size = cols // 2
    half, place_in_half = col // half_size, lax.rem(col, half_size)

    def push(owner_half, into, sems, offset):
        def one(step, carry):
            to = lax.rem(place_in_half + half_size // 2 + step, half_size)
            source = slab.at[offset * cols + owner_half * half_size + to]
            target = into.at[(2 - offset) * half_size + place_in_half]

            def start_remote():
                pltpu.make_async_remote_copy(
                    src_ref=source,
                    dst_ref=target,
                    send_sem=send_sem.at[offset],
                    recv_sem=sems.at[2 - offset],
                    device_id=(band + (offset - 1), half * half_size + to),
                    device_id_type=MESH,
                ).start()

            if offset == 1:
                pl.when(to != place_in_half)(start_remote)
            else:
                start_remote()
            return carry

        lax.fori_loop(0, half_size, one, 0)
        if offset == 1:
            pltpu.make_async_copy(
                slab.at[cols + owner_half * half_size + place_in_half],
                into.at[half_size + place_in_half],
                sems.at[1],
            ).start()

    def place_and_push(offset):
        send(offset)
        push(1 - half, relay, relay_sem, offset)

    for offset in (0, 2, 1):
        pl.when(valid(offset))(functools.partial(place_and_push, offset))
    for offset in (0, 2, 1):
        pl.when(valid(offset))(functools.partial(push, half, recv, recv_sem, offset))

    begin = start[col]
    cos_start, sin_start = begin[0:1], begin[1:2]
    rotated[0] = fine[0] * cos_start - fine[1] * sin_start
    rotated[1] = fine[1] * cos_start + fine[0] * sin_start

    def table_step(step, carry):
        pair = coarse[step]
        cos_base, sin_base = pair[0:1], pair[1:2]
        cos_fine, sin_fine = rotated[0], rotated[1]
        at = pl.ds(pl.multiple_of(step * STEP, STEP), STEP)
        for first, value in (
            (0, cos_base * cos_fine - sin_base * sin_fine),
            (wave_count, sin_base * cos_fine + cos_base * sin_fine),
        ):
            high, low = split(value)
            table_high[at, first : first + wave_count] = high
            table_low[at, first : first + wave_count] = low
        return carry

    lax.fori_loop(0, coarse.shape[0], table_step, 0)

    tiles = sums.shape[1]
    sums[...] = jnp.zeros_like(sums)
    relay_sums[...] = jnp.zeros_like(relay_sums)

    def receive(ref, sems, into, offset):
        here = pl.ds(offset * half_size, half_size)
        pltpu.make_async_copy(ref.at[here], ref.at[here], sems.at[offset]).wait()
        tags = jnp.transpose(
            jnp.concatenate([ref[here, rows, :]] * (-(-8 // half_size)), axis=0)
        )
        wide = lax.broadcasted_iota(jnp.int32, (capacity, tiles), 1).astype(F32)
        chooser = jnp.concatenate(
            [
                (tags[:capacity, source : source + 1] == wide).astype(F32)
                for source in range(half_size)
            ],
            axis=0,
        )
        chooser = jnp.transpose(chooser).astype(BF16)
        incoming = jnp.concatenate(
            [
                ref[here, level * capacity : (level + 1) * capacity, :].reshape(
                    half_size * capacity, LANES
                )
                for level in range(levels)
            ],
            axis=1,
        )
        high, low = split(incoming)
        total = dot(chooser, high) + dot(chooser, low)
        for level in range(levels):
            into[level] += total[:, level * LANES : (level + 1) * LANES]

    for offset in (0, 2, 1):
        pl.when(valid(offset))(functools.partial(receive, relay, relay_sem, relay_sums, offset))
    dense = pl.ds(0, tile_count)
    dense_copy = pltpu.make_async_remote_copy(
        src_ref=relay_sums.at[:, dense],
        dst_ref=passed,
        send_sem=pass_send,
        recv_sem=pass_recv,
        device_id=(band, (1 - half) * half_size + place_in_half),
        device_id_type=MESH,
    )
    dense_copy.start()
    for offset in (0, 2, 1):
        pl.when(valid(offset))(functools.partial(receive, recv, recv_sem, sums, offset))
    dense_copy.wait()
    sums[:, :tile_count, :] += passed[...]

    long_tiles, field_rows = field.shape[:2]
    lat_band = field_rows // levels
    shape3 = (levels, long_tiles, LANES)
    lane3 = lax.broadcasted_iota(jnp.int32, shape3, 2)
    inside = lax.broadcasted_iota(jnp.int32, shape3, 1) * LANES + lane3 < longitudes
    for lat in range(lat_band):
        first, shift = divmod(lat * longitudes, LANES)
        value = sums[:, first : first + long_tiles, :]
        if shift:
            after = sums[:, first + 1 : first + 1 + long_tiles, :]
            value = jnp.where(
                lane3 < LANES - shift,
                pltpu.roll(value, LANES - shift, 2),
                pltpu.roll(after, LANES - shift, 2),
            )
        value = jnp.where(inside, value, 0.0)
        for level in range(levels):
            field[:, level * lat_band + lat, :] = value[level]

    rows_wide = jnp.concatenate([field[tile] for tile in range(long_tiles)], axis=1)
    high, low = split(rows_wide)
    both = dot(jnp.concatenate([high, low], axis=0), table_high[...])
    spectrum = both[:field_rows] + both[field_rows:] + dot(high, table_low[...])
    wave_tiles = spectra.shape[2]
    lat_here = lat_band // cols
    for tile in range(wave_tiles):
        spectra[:, :, tile, :] = spectrum[:, tile * LANES : (tile + 1) * LANES].reshape(
            levels, lat_band, LANES
        )

    def lats(ref, index):
        return ref.at[:, pl.ds(index * lat_here, lat_here)]

    def scatter(to):
        pltpu.make_async_remote_copy(
            src_ref=lats(spectra, to),
            dst_ref=arrived.at[col],
            send_sem=scatter_send,
            recv_sem=scatter_recv,
            device_id=(band, to),
            device_id_type=MESH,
        ).start()

    to_others(scatter)
    pltpu.make_async_copy(lats(spectra, col), arrived.at[col], scatter_recv).start()
    remapped[...] = rows_wide[:, :longitudes].reshape(levels, lat_band, longitudes)
    j = (
        lax.broadcasted_iota(jnp.int32, (wave_tiles, LANES), 0) * LANES
        + lax.broadcasted_iota(jnp.int32, (wave_tiles, LANES), 1)
    )
    wave = jnp.where(j >= wave_count, j - wave_count, j)
    weight = jnp.where(wave == 0, 1.0, 2.0) / period
    gains = [jnp.where(wave <= cutoff[lat], weight, 0.0).astype(F32) for lat in range(lat_here)]
    pltpu.make_async_copy(arrived, arrived, scatter_recv).wait()
    for level in range(levels):
        for lat in range(lat_here):
            total = arrived[0, level, lat]
            for source in range(1, cols):
                total += arrived[source, level, lat]
            scaled[level, lat] = total * gains[lat]

    def spread(to):
        pltpu.make_async_remote_copy(
            src_ref=scaled,
            dst_ref=lats(gathered, col),
            send_sem=spread_send,
            recv_sem=spread_recv,
            device_id=(band, to),
            device_id_type=MESH,
        ).start()

    to_others(spread)
    pltpu.make_async_copy(scaled, lats(gathered, col), spread_recv).start()

    def drain(offset):
        sent = slab.at[pl.ds(0, cols - 2 if offset == 1 else cols)]
        pltpu.make_async_copy(sent, sent, send_sem.at[offset]).wait()

    for offset in range(3):
        pl.when(valid(offset))(functools.partial(drain, offset))
    others = arrived.at[pl.ds(0, cols - 1)]
    pltpu.make_async_copy(others, others, scatter_send).wait()

    pltpu.make_async_copy(spectra, gathered, spread_recv).wait()
    spectrum = jnp.concatenate(
        [gathered[:, :, tile, :].reshape(field_rows, LANES) for tile in range(wave_tiles)], axis=1
    )
    high, low = split(spectrum)
    both = dot(jnp.concatenate([high, low], axis=0), table_high[...], 1, 1)
    result = both[:field_rows] + both[field_rows:] + dot(high, table_low[...], 1, 1)
    filtered[...] = result[:, :longitudes].reshape(levels, lat_band, longitudes)
    pltpu.make_async_copy(others, others, spread_send).wait()


def cos_sin(positions):
    phases = positions[:, None] * np.arange(KW)[None, :] % NLON
    angles = phases * (2 * np.pi / NLON)
    return np.cos(angles).astype(np.float32), np.sin(angles).astype(np.float32)


def local(mesh, source, weights, source_block, owner_device, target_tile, cutoff):
    bands, cols = mesh.shape["band"], mesh.shape["col"]
    levels = source.shape[0]
    block_count, block_width = weights.shape[:2]
    lat_here = cutoff.shape[0]
    lat_band = lat_here * cols
    longitudes = NLON // cols
    cell_count = lat_band * longitudes
    tile_count = (cell_count + block_width - 1) // block_width
    regular = (tile_count + cols - 1) // cols
    capacity = regular + max(1, (block_count - cols * regular + 2 * cols - 1) // (2 * cols))
    capacity = round_up(capacity, 8)
    long_pad = round_up(longitudes, LANES)
    long_tiles = long_pad // LANES
    tiles = round_up(tile_count + long_tiles, LANES)
    fine = np.stack(cos_sin(np.arange(STEP)))
    coarse = np.stack(cos_sin(STEP * np.arange(long_pad // STEP)), axis=1)
    start = np.stack(cos_sin(longitudes * np.arange(cols)), axis=1)

    blocks_here = source.reshape(levels, -1, block_width)
    picked = blocks_here.at[:, source_block.astype(jnp.uint32)].get(mode="promise_in_bounds")
    partial = jnp.einsum("lnb,nbt->nlt", picked, weights, preferred_element_type=F32)
    slab_rows = levels * capacity + 8
    wave_tiles = 2 * KW // LANES
    vmem = pl.BlockSpec(memory_space=pltpu.VMEM)
    shape = jax.ShapeDtypeStruct((levels, lat_band, longitudes), F32)
    return pl.pallas_call(
        functools.partial(remap_kernel, bands, cols, levels, capacity, KW, NLON, longitudes, round_up(tile_count, 8)),
        out_shape=(shape, shape),
        in_specs=[pl.BlockSpec(memory_space=pltpu.SMEM)] + [vmem] * 6,
        out_specs=(vmem, vmem),
        scratch_shapes=[
            pltpu.VMEM((levels, tiles, LANES), F32),
            pltpu.VMEM((long_pad, 2 * KW), BF16),
            pltpu.VMEM((long_pad, 2 * KW), BF16),
            pltpu.VMEM((2, STEP, KW), F32),
            pltpu.VMEM((long_tiles, levels * lat_band, LANES), F32),
            pltpu.VMEM((3 * cols, slab_rows, LANES), F32),
            pltpu.VMEM((3 * cols // 2, slab_rows, LANES), F32),
            pltpu.VMEM((3 * cols // 2, slab_rows, LANES), F32),
            pltpu.VMEM((levels, tiles, LANES), F32),
            pltpu.VMEM((levels, round_up(tile_count, 8), LANES), F32),
            pltpu.VMEM((levels, lat_band, wave_tiles, LANES), F32),
            pltpu.VMEM((cols, levels, lat_here, wave_tiles, LANES), F32),
            pltpu.VMEM((levels, lat_here, wave_tiles, LANES), F32),
            pltpu.VMEM((levels, lat_band, wave_tiles, LANES), F32),
            pltpu.SemaphoreType.DMA((3,)),
            pltpu.SemaphoreType.DMA((3,)),
            pltpu.SemaphoreType.DMA((3,)),
            pltpu.SemaphoreType.DMA,
            pltpu.SemaphoreType.DMA,
            pltpu.SemaphoreType.DMA,
            pltpu.SemaphoreType.DMA,
            pltpu.SemaphoreType.DMA,
            pltpu.SemaphoreType.DMA,
        ],
        compiler_params=pltpu.CompilerParams(has_side_effects=True, vmem_limit_bytes=48 << 20),
    )(
        cutoff,
        partial,
        owner_device.reshape(1, block_count),
        target_tile.reshape(1, block_count),
        fine,
        coarse,
        start,
    )


def solution(mesh):
    in_specs = (
        P(None, ("band", "col")),
        P(("band", "col"), None, None),
        P(("band", "col")),
        P(("band", "col"), None),
        P(("band", "col")),
        P(("band", "col")),
    )
    out_specs = (P(None, "band", "col"), P(None, "band", "col"))
    return jax.shard_map(
        functools.partial(local, mesh),
        mesh=mesh,
        in_specs=in_specs,
        out_specs=out_specs,
        check_vma=False,
    )
```

```python
import functools

import jax
import jax.numpy as jnp
import numpy as np
from jax import lax
from jax.experimental import pallas as pl
from jax.experimental.pallas import tpu as pltpu
from jax.sharding import PartitionSpec as P

NLON = 7200
KW = 512
LANES = 128
STEP = 16
MESH = pl.DeviceIdType.MESH
F32 = jnp.float32
BF16 = jnp.bfloat16


def round_up(value, multiple):
    return (value + multiple - 1) // multiple * multiple


def split(value):
    high = value.astype(BF16)
    return high, (value - high.astype(F32)).astype(BF16)


def dot(left, right, left_dim=1, right_dim=0):
    return lax.dot_general(
        left, right, (((left_dim,), (right_dim,)), ((), ())), preferred_element_type=F32
    )


def remap_kernel(
    bands, cols, levels, capacity, wave_count, period, longitudes, tile_count,
    cutoff, partial, owner_row, tile_row, fine, coarse, start,
    remapped, filtered,
    sums, table_high, table_low, rotated, field, slab, recv, relay, relay_sums, passed,
    spectra, arrived, scaled, gathered,
    send_sem, recv_sem, relay_sem, pass_send, pass_recv,
    scatter_send, scatter_recv, spread_send, spread_recv, cross_recv,
):
    band, col = lax.axis_index("band"), lax.axis_index("col")
    blocks = partial.shape[0]
    rows = levels * capacity
    owners = owner_row[...]
    sublane = lax.broadcasted_iota(jnp.int32, (blocks, blocks), 0)
    lane = lax.broadcasted_iota(jnp.int32, (blocks, blocks), 1)
    owners_wide = jnp.broadcast_to(owners.astype(F32), (8, blocks))
    owner_column = jnp.transpose(owners_wide)[:, 0:1]
    earlier = (owner_column == owners.astype(F32)) & (sublane < lane)
    rank = jnp.sum(earlier.astype(jnp.int32), axis=0, keepdims=True)
    place = owners - (band - 1) * cols
    slot = place * capacity + rank
    data = jnp.concatenate([partial[:, level, :] for level in range(levels)], axis=1)
    stacked = jnp.concatenate(split(data), axis=0)
    slot_lane = lax.broadcasted_iota(jnp.int32, (LANES, blocks), 0)
    tile_at = jnp.where(slot_lane == rank, tile_row[...], 0).astype(F32).astype(BF16)

    def valid(offset):
        target = band + (offset - 1)
        return (target >= 0) & (target < bands)

    def to_others(start_copy):
        def one(step, carry):
            to = lax.rem(col + cols // 2 + step, cols)
            pl.when(to != col)(functools.partial(start_copy, to))
            return carry

        lax.fori_loop(0, cols, one, 0)

    def send(offset):
        group = cols * capacity
        ids = lax.broadcasted_iota(jnp.int32, (group, blocks), 0) + offset * group
        placing = (ids == slot).astype(F32).astype(BF16)
        placed = dot(jnp.concatenate([placing, placing], axis=1), stacked)
        place_ids = lax.broadcasted_iota(jnp.int32, (cols, blocks), 0) + offset * cols
        chosen = (place_ids == place).astype(F32).astype(BF16)
        tags = dot(chosen, tile_at, 1, 1)
        here = pl.ds(offset * cols, cols)
        for level in range(levels):
            piece = placed[:, level * LANES : (level + 1) * LANES]
            slab[here, level * capacity : (level + 1) * capacity, :] = piece.reshape(
                cols, capacity, LANES
            )
        slab[here, rows : rows + 8, :] = jnp.broadcast_to(tags[:, None, :], (cols, 8, LANES))

    half_size = cols // 2
    half, place_in_half = col // half_size, lax.rem(col, half_size)

    def push(owner_half, into, sems, offset):
        def one(step, carry):
            to = lax.rem(place_in_half + half_size // 2 + step, half_size)
            source = slab.at[offset * cols + owner_half * half_size + to]
            target = into.at[(2 - offset) * half_size + place_in_half]

            def start_remote():
                pltpu.make_async_remote_copy(
                    src_ref=source,
                    dst_ref=target,
                    send_sem=send_sem.at[offset],
                    recv_sem=sems.at[2 - offset],
                    device_id=(band + (offset - 1), half * half_size + to),
                    device_id_type=MESH,
                ).start()

            if offset == 1:
                pl.when(to != place_in_half)(start_remote)
            else:
                start_remote()
            return carry

        lax.fori_loop(0, half_size, one, 0)
        if offset == 1:
            pltpu.make_async_copy(
                slab.at[cols + owner_half * half_size + place_in_half],
                into.at[half_size + place_in_half],
                sems.at[1],
            ).start()

    def place_and_push(offset):
        send(offset)
        push(1 - half, relay, relay_sem, offset)

    for offset in (0, 2, 1):
        pl.when(valid(offset))(functools.partial(place_and_push, offset))
    for offset in (0, 2, 1):
        pl.when(valid(offset))(functools.partial(push, half, recv, recv_sem, offset))

    begin = start[col]
    cos_start, sin_start = begin[0:1], begin[1:2]
    rotated[0] = fine[0] * cos_start - fine[1] * sin_start
    rotated[1] = fine[1] * cos_start + fine[0] * sin_start

    def table_step(step, carry):
        pair = coarse[step]
        cos_base, sin_base = pair[0:1], pair[1:2]
        cos_fine, sin_fine = rotated[0], rotated[1]
        at = pl.ds(pl.multiple_of(step * STEP, STEP), STEP)
        for first, value in (
            (0, cos_base * cos_fine - sin_base * sin_fine),
            (wave_count, sin_base * cos_fine + cos_base * sin_fine),
        ):
            high, low = split(value)
            table_high[at, first : first + wave_count] = high
            table_low[at, first : first + wave_count] = low
        return carry

    lax.fori_loop(0, coarse.shape[0], table_step, 0)

    tiles = sums.shape[1]
    sums[...] = jnp.zeros_like(sums)
    relay_sums[...] = jnp.zeros_like(relay_sums)

    def receive(ref, sems, into, offset):
        here = pl.ds(offset * half_size, half_size)
        pltpu.make_async_copy(ref.at[here], ref.at[here], sems.at[offset]).wait()
        tags = jnp.transpose(
            jnp.concatenate([ref[here, rows, :]] * (-(-8 // half_size)), axis=0)
        )
        wide = lax.broadcasted_iota(jnp.int32, (capacity, tiles), 1).astype(F32)
        chooser = jnp.concatenate(
            [
                (tags[:capacity, source : source + 1] == wide).astype(F32)
                for source in range(half_size)
            ],
            axis=0,
        )
        chooser = jnp.transpose(chooser).astype(BF16)
        incoming = jnp.concatenate(
            [
                ref[here, level * capacity : (level + 1) * capacity, :].reshape(
                    half_size * capacity, LANES
                )
                for level in range(levels)
            ],
            axis=1,
        )
        high, low = split(incoming)
        total = dot(chooser, high) + dot(chooser, low)
        for level in range(levels):
            into[level] += total[:, level * LANES : (level + 1) * LANES]

    for offset in (0, 2, 1):
        pl.when(valid(offset))(functools.partial(receive, relay, relay_sem, relay_sums, offset))
    dense = pl.ds(0, tile_count)
    dense_copy = pltpu.make_async_remote_copy(
        src_ref=relay_sums.at[:, dense],
        dst_ref=passed,
        send_sem=pass_send,
        recv_sem=pass_recv,
        device_id=(band, (1 - half) * half_size + place_in_half),
        device_id_type=MESH,
    )
    dense_copy.start()
    for offset in (0, 2, 1):
        pl.when(valid(offset))(functools.partial(receive, recv, recv_sem, sums, offset))
    dense_copy.wait()
    sums[:, :tile_count, :] += passed[...]

    long_tiles, field_rows = field.shape[:2]
    lat_band = field_rows // levels
    shape3 = (levels, long_tiles, LANES)
    lane3 = lax.broadcasted_iota(jnp.int32, shape3, 2)
    inside = lax.broadcasted_iota(jnp.int32, shape3, 1) * LANES + lane3 < longitudes
    for lat in range(lat_band):
        first, shift = divmod(lat * longitudes, LANES)
        value = sums[:, first : first + long_tiles, :]
        if shift:
            after = sums[:, first + 1 : first + 1 + long_tiles, :]
            value = jnp.where(
                lane3 < LANES - shift,
                pltpu.roll(value, LANES - shift, 2),
                pltpu.roll(after, LANES - shift, 2),
            )
        value = jnp.where(inside, value, 0.0)
        for level in range(levels):
            field[:, level * lat_band + lat, :] = value[level]

    rows_wide = jnp.concatenate([field[tile] for tile in range(long_tiles)], axis=1)
    high, low = split(rows_wide)
    both = dot(jnp.concatenate([high, low], axis=0), table_high[...])
    spectrum = both[:field_rows] + both[field_rows:] + dot(high, table_low[...])
    wave_tiles = spectra.shape[2]
    lat_here = lat_band // cols
    for tile in range(wave_tiles):
        spectra[:, :, tile, :] = spectrum[:, tile * LANES : (tile + 1) * LANES].reshape(
            levels, lat_band, LANES
        )

    def lats(ref, index):
        return ref.at[:, pl.ds(index * lat_here, lat_here)]

    def scatter(to):
        pltpu.make_async_remote_copy(
            src_ref=lats(spectra, to),
            dst_ref=arrived.at[col],
            send_sem=scatter_send,
            recv_sem=scatter_recv,
            device_id=(band, to),
            device_id_type=MESH,
        ).start()

    to_others(scatter)
    pltpu.make_async_copy(lats(spectra, col), arrived.at[col], scatter_recv).start()
    remapped[...] = rows_wide[:, :longitudes].reshape(levels, lat_band, longitudes)
    j = (
        lax.broadcasted_iota(jnp.int32, (wave_tiles, LANES), 0) * LANES
        + lax.broadcasted_iota(jnp.int32, (wave_tiles, LANES), 1)
    )
    wave = jnp.where(j >= wave_count, j - wave_count, j)
    weight = jnp.where(wave == 0, 1.0, 2.0) / period
    gains = [jnp.where(wave <= cutoff[lat], weight, 0.0).astype(F32) for lat in range(lat_here)]
    pltpu.make_async_copy(arrived, arrived, scatter_recv).wait()
    for level in range(levels):
        for lat in range(lat_here):
            total = arrived[0, level, lat]
            for source in range(1, cols):
                total += arrived[source, level, lat]
            scaled[level, lat] = total * gains[lat]

    twin_half = (1 - half) * half_size

    def spread(source, owner, to):
        pltpu.make_async_remote_copy(
            src_ref=source,
            dst_ref=lats(gathered, owner),
            send_sem=spread_send,
            recv_sem=spread_recv,
            device_id=(band, to),
            device_id_type=MESH,
        ).start()

    def to_half(source, owner):
        def one(step, carry):
            to = lax.rem(place_in_half + half_size // 2 + step, half_size)
            pl.when(to != place_in_half)(
                lambda: spread(source, owner, half * half_size + to)
            )
            return carry

        lax.fori_loop(0, half_size, one, 0)

    pltpu.make_async_remote_copy(
        src_ref=scaled,
        dst_ref=lats(gathered, col),
        send_sem=spread_send,
        recv_sem=cross_recv,
        device_id=(band, twin_half + place_in_half),
        device_id_type=MESH,
    ).start()
    to_half(scaled, col)
    pltpu.make_async_copy(scaled, lats(gathered, col), spread_recv).start()
    twin = twin_half + place_in_half
    pltpu.make_async_copy(scaled, lats(gathered, twin), cross_recv).wait()
    to_half(lats(gathered, twin), twin)

    def drain(offset):
        sent = slab.at[pl.ds(0, cols - 2 if offset == 1 else cols)]
        pltpu.make_async_copy(sent, sent, send_sem.at[offset]).wait()

    for offset in range(3):
        pl.when(valid(offset))(functools.partial(drain, offset))
    others = arrived.at[pl.ds(0, cols - 1)]
    pltpu.make_async_copy(others, others, scatter_send).wait()

    pltpu.make_async_copy(others, others, spread_recv).wait()
    spectrum = jnp.concatenate(
        [gathered[:, :, tile, :].reshape(field_rows, LANES) for tile in range(wave_tiles)], axis=1
    )
    high, low = split(spectrum)
    both = dot(jnp.concatenate([high, low], axis=0), table_high[...], 1, 1)
    result = both[:field_rows] + both[field_rows:] + dot(high, table_low[...], 1, 1)
    filtered[...] = result[:, :longitudes].reshape(levels, lat_band, longitudes)
    pltpu.make_async_copy(others, others, spread_send).wait()


def cos_sin(positions):
    phases = positions[:, None] * np.arange(KW)[None, :] % NLON
    angles = phases * (2 * np.pi / NLON)
    return np.cos(angles).astype(np.float32), np.sin(angles).astype(np.float32)


def local(mesh, source, weights, source_block, owner_device, target_tile, cutoff):
    bands, cols = mesh.shape["band"], mesh.shape["col"]
    levels = source.shape[0]
    block_count, block_width = weights.shape[:2]
    lat_here = cutoff.shape[0]
    lat_band = lat_here * cols
    longitudes = NLON // cols
    cell_count = lat_band * longitudes
    tile_count = (cell_count + block_width - 1) // block_width
    regular = (tile_count + cols - 1) // cols
    capacity = regular + max(1, (block_count - cols * regular + 2 * cols - 1) // (2 * cols))
    capacity = round_up(capacity, 8)
    long_pad = round_up(longitudes, LANES)
    long_tiles = long_pad // LANES
    tiles = round_up(tile_count + long_tiles, LANES)
    fine = np.stack(cos_sin(np.arange(STEP)))
    coarse = np.stack(cos_sin(STEP * np.arange(long_pad // STEP)), axis=1)
    start = np.stack(cos_sin(longitudes * np.arange(cols)), axis=1)

    blocks_here = source.reshape(levels, -1, block_width)
    picked = blocks_here.at[:, source_block.astype(jnp.uint32)].get(mode="promise_in_bounds")
    partial = jnp.einsum("lnb,nbt->nlt", picked, weights, preferred_element_type=F32)
    slab_rows = levels * capacity + 8
    wave_tiles = 2 * KW // LANES
    vmem = pl.BlockSpec(memory_space=pltpu.VMEM)
    shape = jax.ShapeDtypeStruct((levels, lat_band, longitudes), F32)
    return pl.pallas_call(
        functools.partial(remap_kernel, bands, cols, levels, capacity, KW, NLON, longitudes, round_up(tile_count, 8)),
        out_shape=(shape, shape),
        in_specs=[pl.BlockSpec(memory_space=pltpu.SMEM)] + [vmem] * 6,
        out_specs=(vmem, vmem),
        scratch_shapes=[
            pltpu.VMEM((levels, tiles, LANES), F32),
            pltpu.VMEM((long_pad, 2 * KW), BF16),
            pltpu.VMEM((long_pad, 2 * KW), BF16),
            pltpu.VMEM((2, STEP, KW), F32),
            pltpu.VMEM((long_tiles, levels * lat_band, LANES), F32),
            pltpu.VMEM((3 * cols, slab_rows, LANES), F32),
            pltpu.VMEM((3 * cols // 2, slab_rows, LANES), F32),
            pltpu.VMEM((3 * cols // 2, slab_rows, LANES), F32),
            pltpu.VMEM((levels, tiles, LANES), F32),
            pltpu.VMEM((levels, round_up(tile_count, 8), LANES), F32),
            pltpu.VMEM((levels, lat_band, wave_tiles, LANES), F32),
            pltpu.VMEM((cols, levels, lat_here, wave_tiles, LANES), F32),
            pltpu.VMEM((levels, lat_here, wave_tiles, LANES), F32),
            pltpu.VMEM((levels, lat_band, wave_tiles, LANES), F32),
            pltpu.SemaphoreType.DMA((3,)),
            pltpu.SemaphoreType.DMA((3,)),
            pltpu.SemaphoreType.DMA((3,)),
            pltpu.SemaphoreType.DMA,
            pltpu.SemaphoreType.DMA,
            pltpu.SemaphoreType.DMA,
            pltpu.SemaphoreType.DMA,
            pltpu.SemaphoreType.DMA,
            pltpu.SemaphoreType.DMA,
            pltpu.SemaphoreType.DMA,
        ],
        compiler_params=pltpu.CompilerParams(has_side_effects=True, vmem_limit_bytes=48 << 20),
    )(
        cutoff,
        partial,
        owner_device.reshape(1, block_count),
        target_tile.reshape(1, block_count),
        fine,
        coarse,
        start,
    )


def solution(mesh):
    in_specs = (
        P(None, ("band", "col")),
        P(("band", "col"), None, None),
        P(("band", "col")),
        P(("band", "col"), None),
        P(("band", "col")),
        P(("band", "col")),
    )
    out_specs = (P(None, "band", "col"), P(None, "band", "col"))
    return jax.shard_map(
        functools.partial(local, mesh),
        mesh=mesh,
        in_specs=in_specs,
        out_specs=out_specs,
        check_vma=False,
    )
```
